128 devices in a mesh: light: 8 (over x, z_hi), screen: 16 (over y, z_lo, core).
Axes of the slice: x: 4, y: 4, z: 4 (z_hi: 2, z_lo: 2; z = z_hi * 2 + z_lo), core: 2. Of those that a mesh axis runs over, the one named last changes fastest.
Arguments:
- density: float32 [256, 512, 1024], P('screen', None, 'light'), may hold values from 0 to 1.046875, as said below
- albedo: float32 [256, 512, 1024], P('screen', None, 'light'), may hold values from 0.2 to 1
- light_in: float32 [256, 512], replicated, may hold values from 0.5 to 1.5
- occupancy: int32 [16, 32, 64], P('screen', None, 'light'), may hold values 0 or 1
- phase: int32 [512, 1024], replicated, may hold values from 0 to 15
- fractions: float32 [3, 16], replicated, may hold values from 0 to 1
Outputs:
- image: float32 [512, 1024], P('screen', 'light')
- transmittance: float32 [512, 1024], P('screen', 'light')
- lit_bricks: float32 [256, 512, 1024], P('light', 'screen')
The draws below stay inside these ranges and needn't reach their ends.
Inputs may be any that keep to these rules, and one draw needn't show every extreme that they name: `density`: nonnegative extinction of each cell. `occupancy`: 1 where the brick of 16 cells on a side is occupied.
All inputs are finite; a program needn't handle non-finite values. No bound on the sum of `occupancy` on one device may be relied on, other than what follows from the above.
Results may differ from the reference program's by a relative error of at most 0.0003.
Values sent between devices are 32-bit elements; how exact they have to be, the bound alone decides.
A program may use at most 192 MiB of HBM per device.

```python
import math
import jax
import jax.numpy as jnp
from jax import lax

BRICK = 16
PHASES = 16
NL = 1024
NA = 512
NB = 256


def draw_density(key, part):
    key_rate, key_rough, key_plane, key_patch, key_sheet = jax.random.split(key, 5)
    rate = jnp.exp(jax.random.uniform(key_rate, (NB, NA, 1), jnp.float32, math.log(0.2), math.log(6.0)))
    rough = jnp.exp(jax.random.uniform(key_rough, (NB, NA, NL), jnp.float32, math.log(0.02), math.log(50.0))) / 6.39
    planes = jax.random.randint(key_plane, (3,), 0, NL)
    on_plane = jnp.any(jnp.arange(NL)[None, :] == planes[:, None], axis=0).astype(jnp.float32)
    patch = (jax.random.uniform(key_patch, (NB, NA, NL), jnp.float32) < 0.5).astype(jnp.float32)
    sheet = jax.random.uniform(key_sheet, (NB, NA, NL), jnp.float32, 0.2, 0.7) * patch * on_plane[None, None, :]
    return rate * rough / NL + sheet


def place_ends(entries, own_key, low, top_value):
    extent = entries.shape
    spot = [jax.random.randint(jax.random.fold_in(own_key, axis), (), 0, extent[axis]) for axis in range(len(extent))]
    entries = entries.at[tuple(spot)].set(low)
    longest = extent.index(max(extent))
    spot[longest] = (spot[longest] + 1) % extent[longest]
    return entries.at[tuple(spot)].set(top_value)


def steps_of(rng, dims, shards, smallest, high):
    level = 1.0
    for dim, shards_of in shards:
        draws = jax.random.uniform(jax.random.fold_in(jax.random.fold_in(rng, 6), dim), (shards_of,), jnp.float32, smallest / len(shards), high / len(shards))
        level = level * jnp.repeat(jnp.exp(draws), dims[dim] // shards_of).reshape((-1,) + (1,) * (len(dims) - 1 - dim))
    return level


def setup_inputs(seed: int = 0) -> dict:
    arg_keys = jax.random.split(jax.random.key(seed), 7)
    density = draw_density(jax.random.fold_in(arg_keys[6], 71), 0)
    albedo = jnp.clip(0.2 + 0.8 * jax.random.uniform(arg_keys[1], (NB, NA, NL), jnp.float32) ** steps_of(arg_keys[1], (NB, NA, NL), ((0, 16), (2, 8)), -0.2, 0.2), 0.2, 1.0)
    light_in = jnp.clip(jax.random.uniform(arg_keys[2], (NB, NA), jnp.float32, 0.5, 1.5), 0.5, 1.5)
    occupancy = place_ends((jax.random.randint(arg_keys[3], (NB // BRICK, NA // BRICK, NL // BRICK), 0, 4) < 3).astype(jnp.int32), jax.random.fold_in(arg_keys[3], 1), 0, 1)
    phase = place_ends(jax.random.randint(arg_keys[4], (NA, NL), 0, PHASES), jax.random.fold_in(arg_keys[4], 1), 0, PHASES - 1).astype(jnp.int32)
    fractions = jnp.clip(jax.random.uniform(arg_keys[5], (3, PHASES), jnp.float32, 0.0, 1.0), 0.0, 1.0)
    return {"density": density, "albedo": albedo, "light_in": light_in, "occupancy": occupancy, "phase": phase, "fractions": fractions}


def reference(density, albedo, light_in, occupancy, phase, fractions):
    bricks_b, bricks_a, bricks_l = occupancy.shape
    masked = (density.reshape(bricks_b, BRICK, bricks_a, BRICK, bricks_l, BRICK)
              * occupancy.astype(jnp.float32)[:, None, :, None, :, None]).reshape(density.shape)
    light_depth = jnp.cumsum(masked, axis=2) - masked
    lit_bricks = albedo * light_in[:, :, None] * jnp.exp(-light_depth)
    volumes = jnp.stack([masked, lit_bricks])
    padded = jnp.pad(volumes, ((0, 0), (0, 2), (0, 2), (0, 1)))
    weights = fractions[:, phase]
    tiles = NA // BRICK

    def render(tile):
        zero = jnp.zeros((), jnp.int32)
        start = (tile * BRICK).astype(jnp.int32)
        block = lax.dynamic_slice(padded, (zero, zero, start, zero), (2, NB + 2, BRICK + 2, NL + 1))
        tile_w = lax.dynamic_slice(weights, (zero, start, zero), (3, BRICK, NL))
        sampled = jnp.zeros((2, NB, BRICK, NL), jnp.float32)
        for corner_b in (0, 1):
            for corner_a in (0, 1):
                for corner_l in (0, 1):
                    factor = tile_w[0] if corner_b else 1.0 - tile_w[0]
                    factor = factor * (tile_w[1] if corner_a else 1.0 - tile_w[1])
                    factor = factor * (tile_w[2] if corner_l else 1.0 - tile_w[2])
                    piece = block[:, corner_b:corner_b + NB, corner_a:corner_a + BRICK, corner_l:corner_l + NL]
                    sampled = sampled + factor * piece
        extinct = sampled[0]
        shaded = sampled[1]
        screened = jnp.cumsum(extinct, axis=0) - extinct
        picture = jnp.sum(jnp.exp(-screened) * (1.0 - jnp.exp(-extinct)) * shaded, axis=0)
        passing = jnp.exp(-jnp.sum(extinct, axis=0))
        return picture, passing

    pictures, passings = lax.map(render, jnp.arange(tiles, dtype=jnp.int32))
    return pictures.reshape(NA, NL), passings.reshape(NA, NL), lit_bricks
```

```python
import jax
import jax.numpy as jnp
from jax import lax
from jax.experimental import pallas as pl
from jax.experimental.pallas import tpu as pltpu
from jax.sharding import PartitionSpec as P

MESH = pl.DeviceIdType.MESH
F32 = jnp.float32
BRICK = 16
SB = 16
NA = 512
LW = 128
PAD = 520
DS = (1, 3, 2)


def device(x, y, z, c):
    return (x * 2 + z // 2, y * 4 + (z % 2) * 2 + c)


def bcast(column, rows):
    return jnp.broadcast_to(column, (rows, LW))


def kernel(
    density, albedo, light_in, occ, phase, fractions,
    image_out, passing_out, bricks_out,
    fm, fl, gm, gl, big, w, mask, cform, tform, xbuf, tg, lin, ph, colsend, colrecv,
    img, imgr, img2, img2r, img3, img3r,
    din, ain, small, hs, hr, ts, tr, cs, cr, ys, yr, zs, zr, xs, xr, loc, i1s, i1r, i2s, i2r, i3s, i3r,
):
    li = lax.axis_index("light")
    sj = lax.axis_index("screen")
    x = li // 2
    zh = li % 2
    y = sj // 4
    zl = (sj // 2) % 2
    c = sj % 2
    z = zh * 2 + zl

    def remote(src, dst, ssem, rsem, dev):
        return pltpu.make_async_remote_copy(
            src_ref=src, dst_ref=dst, send_sem=ssem, recv_sem=rsem,
            device_id=dev, device_id_type=MESH,
        )

    def dload(b):
        return pltpu.make_async_copy(density.at[b], fm.at[b, pl.ds(0, NA)], din.at[b])

    def aload(b):
        return pltpu.make_async_copy(albedo.at[b], fl.at[b, pl.ds(0, NA)], ain.at[b])

    lcopy = pltpu.make_async_copy(light_in.at[pl.ds(sj * SB, SB)], lin, small.at[0])
    pcopy = pltpu.make_async_copy(phase.at[:, pl.ds(li * LW, LW)], ph, small.at[1])
    for b in range(SB):
        dload(b).start()
        aload(b).start()
    lcopy.start()
    pcopy.start()

    barrier = pltpu.get_barrier_semaphore()
    near = [(lax.rem(li + i, 8), sj) for i in range(1, 8)]
    near += [device(x, lax.rem(y + d, 4), z, c) for d in (1, 2, 3)]
    near += [device(lax.rem(x + d, 4), y, z, 1 - c) for d in range(4)]
    near += [device(x, y, lax.rem(z + d, 4), c) for d in (1, 2, 3)]
    near += [(li, lax.rem(sj + 1, 16)), (li, lax.rem(sj + 15, 16))]
    for dev in near:
        pl.semaphore_signal(barrier, inc=1, device_id=dev, device_id_type=MESH)

    lane = lax.broadcasted_iota(jnp.int32, (128, LW), 1)
    o = occ[0].astype(F32)
    spread = (
        lax.broadcasted_iota(jnp.int32, (8, LW), 1) // BRICK
        == lax.broadcasted_iota(jnp.int32, (8, LW), 0)
    ).astype(F32)
    wide = jnp.dot(o, spread, preferred_element_type=F32)
    tall = (
        lax.broadcasted_iota(jnp.int32, (NA, 32), 0) // BRICK
        == lax.broadcasted_iota(jnp.int32, (NA, 32), 1)
    ).astype(F32)
    mask[...] = jnp.dot(tall, wide, preferred_element_type=F32)
    r = lax.broadcasted_iota(jnp.int32, (256, 256), 0) % LW
    q = lax.broadcasted_iota(jnp.int32, (256, 256), 1)
    upper = jnp.logical_or(r < q, q >= LW).astype(jnp.bfloat16)

    zero8 = jnp.zeros((8, LW), F32)
    for b in range(SB + 1):
        for ref in (fm, fl, gm, gl):
            ref[b, NA:PAD, :] = zero8

    def first(b, _):
        dload(b).wait()
        aload(b).wait()
        for t in range(4):
            rows = pl.ds(t * 128, 128)
            m = fm[b, rows, :] * mask[rows, :]
            fm[b, rows, :] = m
            hi = m.astype(jnp.bfloat16)
            lo = (m - hi.astype(F32)).astype(jnp.bfloat16)
            both = jnp.dot(
                jnp.concatenate([hi, lo], axis=1), upper, preferred_element_type=F32
            )
            fl[b, rows, :] = fl[b, rows, :] * jnp.exp(-both[:, :LW])
            cform[0, rows, :] = jnp.where(lane == b, both[:, LW:], cform[0, rows, :])
        return 0

    lax.fori_loop(0, SB, first, 0)
    for t in range(4):
        cols = pl.ds(t * 128, 128)
        tg[li, :, cols] = cform[0, cols, :].T[:SB, :]

    pl.semaphore_wait(barrier, len(near))

    def tcopy(i):
        dev = (lax.rem(li + i, 8), sj)
        return remote(tg.at[li], tg.at[li], ts.at[i], tr.at[li], dev)

    for i in (4, 3, 5, 2, 6, 1, 7):
        tcopy(i).start()

    def halo(f, slot):
        return remote(
            f.at[0, pl.ds(0, NA)], f.at[SB, pl.ds(0, NA)], hs.at[slot], hr.at[slot],
            (li, lax.rem(sj + 15, 16)),
        )

    @pl.when(sj > 0)
    def _():
        halo(fm, 0).start()

    @pl.when(sj == 15)
    def _():
        for t in range(4):
            fm[SB, t * 128 : (t + 1) * 128, :] = jnp.zeros((128, LW), F32)
            fl[SB, t * 128 : (t + 1) * 128, :] = jnp.zeros((128, LW), F32)

    pcopy.wait()

    def weigh(t, _):
        rows = pl.ds(pl.multiple_of(t * 32, 32), 32)
        p = ph[rows, :]
        for k in range(3):
            v = jnp.full((32, LW), fractions[k, 0], F32)
            for level in range(1, 16):
                v = jnp.where(p == level, fractions[k, level], v)
            w[k, rows, :] = v
        return 0

    lax.fori_loop(0, 16, weigh, 0)
    xbuf[...] = jnp.zeros_like(xbuf)
    lcopy.wait()

    for i in range(1, 8):
        src = lax.rem(li + i, 8)
        remote(tg.at[src], tg.at[src], ts.at[i], tr.at[src], (src, sj)).wait_recv()
    before = jnp.zeros((SB, NA), F32)
    for i in range(8):
        before = before + jnp.where(i < li, tg[i], 0.0)
    xbuf[0:SB, :] = lin[...] * jnp.exp(-before)
    for t in range(4):
        cols = pl.ds(t * 128, 128)
        cform[0, cols, :] = xbuf[:, cols].T

    def unit(d, qq, kz):
        return (d * 4 + qq) * 2 + kz

    def held(d):
        return d if d == 0 else d + 3

    def ycopy(d, qq):
        return remote(
            big.at[pl.ds(unit(d, qq, 0), 2)], big.at[pl.ds(unit(d + 3, qq, 0), 2)],
            ys.at[d, qq], yr.at[d, qq], device(x, lax.rem(y + d, 4), z, c),
        )

    def zcopy(d, qq, kz):
        zz = 2 * zl + kz
        return zz, remote(
            big.at[unit(held(d), qq, kz)], big.at[56 + (zh * 4 + d) * 4 + qq],
            zs.at[d, qq, kz], zr.at[zh, d, qq], device(x, y, zz, c),
        )

    def zsend(d, qq):
        for kz in range(2):
            zz, cp = zcopy(d, qq, kz)

            @pl.when(zz != z)
            def _():
                cp.start()

    def mine(j):
        return (1 - (zl + zh) % 2) * (1 - (j + zh) % 2)

    def zwait(j, d, qq):
        @pl.when(mine(j) == 0)
        def _():
            place = big.at[56 + (j * 4 + d) * 4 + qq]
            remote(place, place, zs.at[d, qq, 0], zr.at[j, d, qq], device(x, y, z, 1 - c)).wait_recv()

    def xcopies(j, d, qq, kc):
        own = mine(j)
        at = own * unit(held(d), qq, zl) + (1 - own) * (56 + (j * 4 + d) * 4 + qq)
        src = big.at[at, pl.ds(kc * 128, 128)]
        slot = (x * 2 + j) * 2 + c
        xx = lax.rem(y + 4 - d, 4)
        here = jnp.logical_and(xx == x, c == kc)
        dst = bricks_out.at[slot, qq]
        far = remote(src, dst, xs.at[j, d, qq, kc], xr.at[slot, qq], device(xx, y, z, kc))
        near_ = pltpu.make_async_copy(src, dst, loc.at[j, qq])
        return here, near_, far

    def xsend(d, qq):
        for j in range(2):
            zwait(j, d, qq)
            for kc in range(2):
                here, near_, far = xcopies(j, d, qq, kc)

                @pl.when(here)
                def _():
                    near_.start()

                @pl.when(jnp.logical_not(here))
                def _():
                    far.start()

    for b in range(SB):
        qq, bb = b // 4, b % 4
        for d in range(4):
            yy = lax.rem(y + d, 4)
            rows = pl.ds(pl.multiple_of(yy * 128, 128), 128)
            v = fl[b, rows, :] * bcast(cform[0, rows, b : b + 1], 128)
            fl[b, rows, :] = v
            for k in range(4):
                big[unit(d, qq, k // 2), (k % 2) * 128 + bb * 32 : (k % 2) * 128 + bb * 32 + 32, :] = v[
                    k * 32 : k * 32 + 32, :
                ]
        if b == 0:
            @pl.when(sj > 0)
            def _():
                halo(fl, 1).start()
        if bb == 3:
            for d in DS:
                ycopy(d, qq).start()
            zsend(0, qq)

    def ystep(d, qq):
        place = big.at[pl.ds(unit(d + 3, qq, 0), 2)]
        remote(place, place, ys.at[d, qq], yr.at[d, qq], device(x, lax.rem(y + d, 4), z, c)).wait_recv()
        zsend(d, qq)

    def halo_wait():
        @pl.when(sj < 15)
        def _():
            for slot, f in enumerate((fm, fl)):
                place = f.at[SB, pl.ds(0, NA)]
                remote(place, place, hs.at[slot], hr.at[slot], (li, lax.rem(sj + 1, 16))).wait_recv()

    def ccopy():
        return remote(colsend, colrecv, cs, cr, (lax.rem(li + 7, 8), sj))

    def columns():
        for f, ref in enumerate((fm, fl)):
            def gather(t, _):
                rows = pl.ds(pl.multiple_of(t * 32, 32), 32)
                acc = jnp.zeros((32, LW), F32)
                for b in range(SB + 1):
                    acc = jnp.where(lane[:32] == b, bcast(ref[b, rows, 0:1], 32), acc)
                cform[f, rows, :] = acc
                return 0

            lax.fori_loop(0, 16, gather, 0)
            for t in range(4):
                cols = pl.ds(t * 128, 128)
                colsend[f, :, cols] = cform[f, cols, :].T[:24, :]

        @pl.when(li > 0)
        def _():
            ccopy().start()

        @pl.when(li == 7)
        def _():
            colrecv[...] = jnp.zeros_like(colrecv)

    def column_wait():
        @pl.when(li < 7)
        def _():
            remote(colrecv, colrecv, cs, cr, (lax.rem(li + 1, 8), sj)).wait_recv()
        for f in range(2):
            xbuf[0:24, :] = colrecv[f]
            for t in range(4):
                cols = pl.ds(t * 128, 128)
                cform[f, cols, :] = xbuf[:, cols].T

    def shifted(t, _):
        rows = pl.ds(pl.multiple_of(t * 32, 32), 32)
        for f, (src, dst) in enumerate(((fm, gm), (fl, gl))):
            edge = cform[f, rows, :]
            for b in range(SB + 1):
                rolled = pltpu.roll(src[b, rows, :], LW - 1, 1)
                dst[b, rows, :] = jnp.where(lane[:32] == LW - 1, bcast(edge[:, b : b + 1], 32), rolled)
        return 0

    def march(t, _):
        a0 = pl.multiple_of(t * 32, 32)
        rows = pl.ds(a0, 32)
        after = pl.ds(a0 + 1, 32)
        wb, wa, wl = w[0, rows, :], w[1, rows, :], w[2, rows, :]

        def mixed(f, g, b):
            f0 = f[b, rows, :]
            g0 = g[b, rows, :]
            near = f0 + wa * (f[b, after, :] - f0)
            further = g0 + wa * (g[b, after, :] - g0)
            return near + wl * (further - near)

        m0, s0 = mixed(fm, gm, 0), mixed(fl, gl, 0)
        passing = jnp.ones((32, LW), F32)
        part = jnp.zeros((32, LW), F32)
        for b in range(1, SB + 1):
            m1, s1 = mixed(fm, gm, b), mixed(fl, gl, b)
            extinct = m0 + wb * (m1 - m0)
            shaded = s0 + wb * (s1 - s0)
            left = passing * jnp.exp(-extinct)
            part = part + (passing - left) * shaded
            passing = left
            m0, s0 = m1, s1
        place = pl.ds(pl.multiple_of((t // 2) * 32, 32), 32)
        img[t % 2, 0, place, :] = part
        img[t % 2, 1, place, :] = passing
        return 0

    def joined(front, own, other):
        p0 = jnp.where(front, own[0], other[0])
        p1 = jnp.where(front, other[0], own[0])
        t0 = jnp.where(front, own[1], other[1])
        return p0 + t0 * p1, own[1] * other[1]

    def i1copy():
        return remote(img.at[1 - c], imgr, i1s, i1r, device(x, y, z, 1 - c))

    def i2copy():
        return remote(img2.at[1 - zl], img2r, i2s, i2r, device(x, y, zh * 2 + 1 - zl, c))

    def i3copy(d):
        yy = lax.rem(y + d, 4)
        return remote(img3.at[yy], img3r.at[y], i3s.at[d], i3r.at[y], device(x, yy, z, c))

    def image1():
        i1copy().wait_recv()
        for yy in range(4):
            for zz in range(2):
                rows = slice((yy * 2 + zz) * 32, (yy * 2 + zz) * 32 + 32)
                own = (img[c, 0, rows, :], img[c, 1, rows, :])
                a, t = joined(c == 0, own, (imgr[0, rows, :], imgr[1, rows, :]))
                img2[zz, 0, yy * 32 : yy * 32 + 32, :] = a
                img2[zz, 1, yy * 32 : yy * 32 + 32, :] = t
        i2copy().start()

    def image2():
        i2copy().wait_recv()
        for yy in range(4):
            rows = slice(yy * 32, yy * 32 + 32)
            own = (img2[zl, 0, rows, :], img2[zl, 1, rows, :])
            a, t = joined(zl == 0, own, (img2r[0, rows, :], img2r[1, rows, :]))
            img3[yy, 0, :, :] = a
            img3[yy, 1, :, :] = t
        for d in DS:
            i3copy(d).start()
        img3r[y] = img3[y]

    def image3():
        for d in DS:
            src = lax.rem(y + d, 4)
            remote(img3r.at[src], img3r.at[src], i3s.at[d], i3r.at[src], device(x, src, z, c)).wait_recv()
        a, t = img3r[0, 0], img3r[0, 1]
        for yy in range(1, 4):
            a = a + t * img3r[yy, 0]
            t = t * img3r[yy, 1]
        image_out[...] = a
        passing_out[...] = t

    def run(body, lo, hi):
        return lambda: lax.fori_loop(lo, hi, body, 0)

    work = {
        (0, 2): [halo_wait, columns],
        (1, 0): [column_wait, run(shifted, 0, 5)],
        (1, 1): [run(shifted, 5, 11)],
        (1, 2): [run(shifted, 11, 16)],
        (1, 3): [run(march, 0, 3)],
        (2, 0): [run(march, 3, 6)],
        (2, 1): [run(march, 6, 9)],
        (2, 2): [run(march, 9, 12)],
        (2, 3): [run(march, 12, 16), lambda: i1copy().start()],
        (3, 0): [image1],
        (3, 1): [image2],
        (3, 2): [image3],
    }
    order = [(qq, i) for qq in range(4) for i in range(4)]
    hops = (0,) + DS
    last = None
    for qq, i in order:
        if hops[i]:
            ystep(hops[i], qq)
        if last is not None:
            xsend(*last)
        last = (hops[i], qq)
        for task in work.get((qq, i), ()):
            task()
    xsend(*last)

    @pl.when(sj > 0)
    def _():
        halo(fm, 0).wait_send()
        halo(fl, 1).wait_send()

    for i in range(1, 8):
        tcopy(i).wait_send()

    @pl.when(li > 0)
    def _():
        ccopy().wait_send()

    i1copy().wait_send()
    i2copy().wait_send()
    for d in DS:
        i3copy(d).wait_send()
    for qq in range(4):
        for d in DS:
            ycopy(d, qq).wait_send()
        for d in range(4):
            for kz in range(2):
                zz, cp = zcopy(d, qq, kz)

                @pl.when(zz != z)
                def _():
                    cp.wait_send()

            for j in range(2):
                for kc in range(2):
                    here, near_, far = xcopies(j, d, qq, kc)

                    @pl.when(here)
                    def _():
                        near_.wait()

                    @pl.when(jnp.logical_not(here))
                    def _():
                        far.wait_send()

        for sx in range(4):
            for j in range(2):
                for sc in range(2):
                    slot = (sx * 2 + j) * 2 + sc
                    here = jnp.logical_and(sx == x, sc == c)

                    @pl.when(jnp.logical_not(here))
                    def _():
                        place = bricks_out.at[slot, qq]
                        remote(place, place, xs.at[0, 0, 0, 0], xr.at[slot, qq], device(x, y, z, 1 - c)).wait_recv()


def placed(src, out):
    out[...] = src[...].reshape(32, 32, LW)


def local(density, albedo, light_in, occupancy, phase, fractions):
    anywhere = pl.BlockSpec(memory_space=pl.ANY)
    vmem = pl.BlockSpec(memory_space=pltpu.VMEM)
    dma = pltpu.SemaphoreType.DMA
    image, passing, bricks = pl.pallas_call(
        kernel,
        out_shape=(
            jax.ShapeDtypeStruct((32, LW), F32),
            jax.ShapeDtypeStruct((32, LW), F32),
            jax.ShapeDtypeStruct((16, 4, 128, LW), F32),
        ),
        in_specs=[anywhere, anywhere, anywhere, vmem, anywhere, pl.BlockSpec(memory_space=pltpu.SMEM)],
        out_specs=(vmem, vmem, anywhere),
        scratch_shapes=[
            pltpu.VMEM((SB + 1, PAD, LW), F32),
            pltpu.VMEM((SB + 1, PAD, LW), F32),
            pltpu.VMEM((SB + 1, PAD, LW), F32),
            pltpu.VMEM((SB + 1, PAD, LW), F32),
            pltpu.VMEM((88, 256, LW), F32),
            pltpu.VMEM((3, NA, LW), F32),
            pltpu.VMEM((NA, LW), F32),
            pltpu.VMEM((2, NA, LW), F32),
            pltpu.VMEM((8, LW), F32),
            pltpu.VMEM((128, NA), F32),
            pltpu.VMEM((8, SB, NA), F32),
            pltpu.VMEM((SB, NA), F32),
            pltpu.VMEM((NA, LW), jnp.int32),
            pltpu.VMEM((2, 24, NA), F32),
            pltpu.VMEM((2, 24, NA), F32),
            pltpu.VMEM((2, 2, 256, LW), F32),
            pltpu.VMEM((2, 256, LW), F32),
            pltpu.VMEM((2, 2, 128, LW), F32),
            pltpu.VMEM((2, 128, LW), F32),
            pltpu.VMEM((4, 2, 32, LW), F32),
            pltpu.VMEM((4, 2, 32, LW), F32),
            dma((SB,)), dma((SB,)), dma((2,)),
            dma((2,)), dma((2,)), dma((8,)), dma((8,)), dma(()), dma(()),
            dma((4, 4)), dma((4, 4)), dma((4, 4, 2)), dma((2, 4, 4)),
            dma((2, 4, 4, 2)), dma((16, 4)), dma((2, 4)),
            dma(()), dma(()), dma(()), dma(()), dma((4,)), dma((4,)),
        ],
        compiler_params=pltpu.CompilerParams(
            collective_id=0, has_side_effects=True, vmem_limit_bytes=60 << 20
        ),
    )(density, albedo, light_in, occupancy, phase, fractions)
    bricks = bricks.reshape(16, 16, 32, LW)
    lit = pl.pallas_call(
        placed,
        grid=(8,),
        out_shape=jax.ShapeDtypeStruct((32, 32, 1024), F32),
        in_specs=[pl.BlockSpec((2, 16, 32, LW), lambda i: (i, 0, 0, 0))],
        out_specs=pl.BlockSpec((32, 32, LW), lambda i: (0, 0, i)),
    )(bricks)
    return image, passing, lit


def solution(mesh):
    return jax.shard_map(
        local,
        mesh=mesh,
        in_specs=(
            P("screen", None, "light"),
            P("screen", None, "light"),
            P(),
            P("screen", None, "light"),
            P(),
            P(),
        ),
        out_specs=(P("screen", "light"), P("screen", "light"), P("light", "screen", None)),
        check_vma=False,
    )
```

```python
import jax
import jax.numpy as jnp
from jax import lax
from jax.experimental import pallas as pl
from jax.experimental.pallas import tpu as pltpu
from jax.sharding import PartitionSpec as P

MESH = pl.DeviceIdType.MESH
F32 = jnp.float32
BRICK = 16
SB = 16
NA = 512
LW = 128
PAD = 520
DS = (1, 3, 2)
Q = 8
LAG = 5


def device(x, y, z, c):
    return (x * 2 + z // 2, y * 4 + (z % 2) * 2 + c)


def bcast(column, rows):
    return jnp.broadcast_to(column, (rows, LW))


def kernel(
    density, albedo, light_in, occ, phase, fractions,
    image_out, passing_out, factor_out, bricks_out,
    fm, fl, gm, gl, big, w, mask, cform, xbuf, cbuf, tg, lin, lin2, ph, colsend, colrecv,
    tb, tin, ftmp, img, imgr, img2, img2r, img3, img3r,
    din, ain, small, hs, hr, ts, tr, es, er, cs, cr, ys, yr, zs, zr, xs, xr, loc,
    tys, tyr, tzs, tzr, txs, txr, i1s, i1r, i2s, i2r, i3s, i3r,
):
    li = lax.axis_index("light")
    sj = lax.axis_index("screen")
    x = li // 2
    zh = li % 2
    y = sj // 4
    zl = (sj // 2) % 2
    c = sj % 2
    z = zh * 2 + zl

    def remote(src, dst, ssem, rsem, dev):
        return pltpu.make_async_remote_copy(
            src_ref=src, dst_ref=dst, send_sem=ssem, recv_sem=rsem,
            device_id=dev, device_id_type=MESH,
        )

    def dload(b):
        return pltpu.make_async_copy(density.at[b], fm.at[b, pl.ds(0, NA)], din.at[b])

    def aload(b):
        return pltpu.make_async_copy(albedo.at[b], fl.at[b, pl.ds(0, NA)], ain.at[b])

    lcopy = pltpu.make_async_copy(light_in.at[pl.ds(sj * SB, SB)], lin, small.at[0])
    pcopy = pltpu.make_async_copy(phase.at[:, pl.ds(li * LW, LW)], ph, small.at[1])
    l2copy = pltpu.make_async_copy(
        light_in.at[pl.ds(li * 32, 32), pl.ds(y * LW, LW)], lin2, small.at[2]
    )
    for b in range(SB):
        dload(b).start()
        aload(b).start()
    lcopy.start()
    l2copy.start()
    pcopy.start()

    barrier = pltpu.get_barrier_semaphore()
    near = [(lax.rem(li + i, 8), sj) for i in range(1, 8)]
    near += [device(x, lax.rem(y + d, 4), z, c) for d in (1, 2, 3)]
    near += [device(lax.rem(x + d, 4), y, z, 1 - c) for d in range(4)]
    near += [device(x, y, lax.rem(z + d, 4), c) for d in (1, 2, 3)]
    near += [(li, lax.rem(sj + 1, 16)), (li, lax.rem(sj + 15, 16))]
    for dev in near:
        pl.semaphore_signal(barrier, inc=1, device_id=dev, device_id_type=MESH)

    lane = lax.broadcasted_iota(jnp.int32, (128, LW), 1)
    o = occ[0].astype(F32)
    tall = (
        lax.broadcasted_iota(jnp.int32, (NA, 32), 0) // BRICK
        == lax.broadcasted_iota(jnp.int32, (NA, 32), 1)
    ).astype(F32)
    tall = lax.dot_general(tall, o, (((1,), (1,)), ((), ())), preferred_element_type=F32)
    spread = (
        lax.broadcasted_iota(jnp.int32, (8, LW), 1) // BRICK
        == lax.broadcasted_iota(jnp.int32, (8, LW), 0)
    ).astype(F32)
    mask[...] = jnp.dot(tall, spread, preferred_element_type=F32)
    r = lax.broadcasted_iota(jnp.int32, (256, 256), 0) % LW
    q = lax.broadcasted_iota(jnp.int32, (256, 256), 1)
    upper = jnp.logical_or(r < q, q >= LW).astype(jnp.bfloat16)

    def unit(d, qq, kz):
        return (d * Q + qq) * 2 + kz

    def held(d):
        return d if d == 0 else d + 3

    def middle(j, d, qq):
        return 14 * Q + (j * 4 + d) * Q + qq

    def ydev(d):
        return device(x, lax.rem(y + d, 4), z, c)

    def ycopy(d, qq):
        return remote(
            big.at[pl.ds(unit(d, qq, 0), 2)], big.at[pl.ds(unit(d + 3, qq, 0), 2)],
            ys.at[d, qq], yr.at[d, qq], ydev(d),
        )

    def ysend(qq):
        for d in DS:
            ycopy(d, qq).start()

    def halo(f, slot):
        return remote(
            f.at[0, pl.ds(0, NA)], f.at[SB, pl.ds(0, NA)], hs.at[slot], hr.at[slot],
            (li, lax.rem(sj + 15, 16)),
        )

    def first(qq):
        for bb in range(2):
            b = qq * 2 + bb
            dload(b).wait()
            aload(b).wait()
            for d in range(4):
                yy = lax.rem(y + d, 4)
                rows = pl.ds(pl.multiple_of(yy * 128, 128), 128)
                m = fm[b, rows, :] * mask[rows, :]
                fm[b, rows, :] = m
                hi = m.astype(jnp.bfloat16)
                lo = (m - hi.astype(F32)).astype(jnp.bfloat16)
                both = jnp.dot(
                    jnp.concatenate([hi, lo], axis=1), upper, preferred_element_type=F32
                )
                v = fl[b, rows, :] * jnp.exp(-both[:, :LW])
                fl[b, rows, :] = v
                for k in range(4):
                    to = (k % 2) * 64 + bb * 32
                    big[unit(d, qq, k // 2), to : to + 32, :] = v[k * 32 : k * 32 + 32, :]
                cform[0, rows, :] = jnp.where(lane == b, both[:, LW:], cform[0, rows, :])

    def weigh(t, _):
        rows = pl.ds(pl.multiple_of(t * 32, 32), 32)
        p = ph[rows, :]
        for k in range(3):
            v = jnp.full((32, LW), fractions[k, 0], F32)
            for level in range(1, 16):
                v = jnp.where(p == level, fractions[k, level], v)
            w[k, rows, :] = v
        return 0

    first(0)
    pcopy.wait()
    lax.fori_loop(0, 16, weigh, 0)
    pl.semaphore_wait(barrier, len(near))
    @pl.when(sj > 0)
    def _():
        halo(fm, 0).start()
        halo(fl, 1).start()

    ysend(0)
    first(1)
    ysend(1)

    @pl.when(sj == 15)
    def _():
        for t in range(4):
            fm[SB, t * 128 : (t + 1) * 128, :] = jnp.zeros((128, LW), F32)
            fl[SB, t * 128 : (t + 1) * 128, :] = jnp.zeros((128, LW), F32)
        xbuf[SB:24, :] = jnp.zeros((8, NA), F32)

    first(2)

    def rest(qq, _):
        first(qq)
        return 0

    lax.fori_loop(3, Q, rest, 0)
    for t in range(4):
        cols = pl.ds(t * 128, 128)
        totals = cform[0, cols, :].T[:SB, :]
        tg[li, :, cols] = totals
        tb[lax.rem(t + 4 - y, 4)] = totals

    def tcopy(i):
        dev = (lax.rem(li + i, 8), sj)
        return remote(tg.at[li], tg.at[li], ts.at[i], tr.at[li], dev)

    def tycopy(d):
        return remote(tb.at[d], tb.at[d + 3], tys.at[d], tyr.at[d], ydev(d))

    for i in (4, 3, 5, 2, 6, 1, 7):
        tcopy(i).start()
    for d in DS:
        tycopy(d).start()

    zero8 = jnp.zeros((8, LW), F32)
    for b in range(SB + 1):
        for ref in (fm, fl, gm, gl):
            ref[b, NA:PAD, :] = zero8

    def zcopy(d, qq, kz):
        zz = 2 * zl + kz
        return zz, remote(
            big.at[unit(held(d), qq, kz)], big.at[middle(zh, d, qq)],
            zs.at[d, qq, kz], zr.at[zh, d, qq], device(x, y, zz, c),
        )

    def tzcopy(d, kz):
        zz = 2 * zl + kz
        return zz, remote(
            tb.at[held(d)], tb.at[7 + zh * 4 + d], tzs.at[d, kz], tzr.at[zh, d],
            device(x, y, zz, c),
        )

    def zsend(d, qq):
        for kz in range(2):
            zz, cp = zcopy(d, qq, kz)

            @pl.when(zz != z)
            def _():
                cp.start()

    def mine(j):
        return (1 - (zl + zh) % 2) * (1 - (j + zh) % 2)

    def zwait(j, d, qq):
        @pl.when(mine(j) == 0)
        def _():
            place = big.at[middle(j, d, qq)]
            remote(place, place, zs.at[d, qq, 0], zr.at[j, d, qq], device(x, y, z, 1 - c)).wait_recv()

    def xto(j, d, kc):
        xx = lax.rem(y + 4 - d, 4)
        here = jnp.logical_and(xx == x, c == kc)
        return (x * 2 + j) * 2 + c, here, device(xx, y, z, kc)

    def xcopies(j, d, qq, kc):
        own = mine(j)
        at = own * unit(held(d), qq, zl) + (1 - own) * middle(j, d, qq)
        src = big.at[at, pl.ds(kc * 64, 64)]
        slot, here, dev = xto(j, d, kc)
        dst = bricks_out.at[slot, qq]
        far = remote(src, dst, xs.at[j, d, qq, kc], xr.at[slot, qq], dev)
        near_ = pltpu.make_async_copy(src, dst, loc.at[j, qq])
        return here, near_, far

    def xsend(d, qq):
        for j in range(2):
            zwait(j, d, qq)
            for kc in range(2):
                here, near_, far = xcopies(j, d, qq, kc)

                @pl.when(here)
                def _():
                    near_.start()

                @pl.when(jnp.logical_not(here))
                def _():
                    far.start()

    def ystep(d, qq):
        if d:
            place = big.at[pl.ds(unit(d + 3, qq, 0), 2)]
            remote(place, place, ys.at[d, qq], yr.at[d, qq], ydev(d)).wait_recv()
        zsend(d, qq)

    def totals_z():
        for d in DS:
            remote(tb.at[d + 3], tb.at[d + 3], tys.at[d], tyr.at[d], ydev(d)).wait_recv()
        for d in range(4):
            for kz in range(2):
                zz, cp = tzcopy(d, kz)

                @pl.when(zz != z)
                def _():
                    cp.start()

    def txcopy(j, d, kc):
        own = mine(j)
        at = own * held(d) + (1 - own) * (7 + j * 4 + d)
        slot, here, dev = xto(j, d, kc)
        return at, slot, here, remote(tb.at[at], tin.at[slot], txs.at[j, d, kc], txr.at[slot], dev)

    def totals_x():
        for j in range(2):
            for d in range(4):
                @pl.when(mine(j) == 0)
                def _():
                    place = tb.at[7 + j * 4 + d]
                    remote(place, place, tzs.at[d, 0], tzr.at[j, d], device(x, y, z, 1 - c)).wait_recv()

                for kc in range(2):
                    at, slot, here, far = txcopy(j, d, kc)

                    @pl.when(here)
                    def _():
                        tin[slot] = tb[at]

                    @pl.when(jnp.logical_not(here))
                    def _():
                        far.start()

    def arrivals(wait):
        for sx in range(4):
            for j in range(2):
                for sc in range(2):
                    slot = (sx * 2 + j) * 2 + sc
                    here = jnp.logical_and(sx == x, sc == c)

                    @pl.when(jnp.logical_not(here))
                    def _():
                        wait(slot)

    def factors():
        def wait(slot):
            remote(tin.at[slot], tin.at[slot], txs.at[0, 0, 0], txr.at[slot], device(x, y, z, 1 - c)).wait_recv()

        arrivals(wait)
        l2copy.wait()
        for cc in range(2):
            above = jnp.zeros((SB, LW), F32)
            for i in range(8):
                ftmp[i * SB : i * SB + SB, :] = lin2[cc * SB : cc * SB + SB, :] * jnp.exp(-above)
                above = above + tin[i * 2 + cc]
            cform[0, 0:128, :] = ftmp[...].T
            factor_out[cc] = cform[0, pl.ds(pl.multiple_of((zl * 2 + c) * 32, 32), 32), :]

    def ecopy():
        return remote(
            xbuf.at[pl.ds(0, 8)], xbuf.at[pl.ds(SB, 8)], es, er, (li, lax.rem(sj + 15, 16))
        )

    def reach():
        lcopy.wait()
        for i in range(1, 8):
            src = lax.rem(li + i, 8)
            remote(tg.at[src], tg.at[src], ts.at[i], tr.at[src], (src, sj)).wait_recv()
        before = jnp.zeros((SB, NA), F32)
        for i in range(8):
            before = before + jnp.where(i < li, tg[i], 0.0)
        xbuf[0:SB, :] = lin[...] * jnp.exp(-before)

        @pl.when(sj > 0)
        def _():
            ecopy().start()

    def halo_wait():
        @pl.when(sj > 0)
        def _():
            halo(fm, 0).wait_send()
            halo(fl, 1).wait_send()

        @pl.when(sj < 15)
        def _():
            for slot, f in enumerate((fm, fl)):
                place = f.at[SB, pl.ds(0, NA)]
                remote(place, place, hs.at[slot], hr.at[slot], (li, lax.rem(sj + 1, 16))).wait_recv()
            place = xbuf.at[pl.ds(SB, 8)]
            remote(place, place, es, er, (li, lax.rem(sj + 1, 16))).wait_recv()

        for t in range(4):
            cols = pl.ds(t * 128, 128)
            cform[0, cols, :] = xbuf[:, cols].T

    def scale(t, _):
        rows = pl.ds(pl.multiple_of(t * 32, 32), 32)
        e = cform[0, rows, :]
        am = jnp.zeros((32, LW), F32)
        al = jnp.zeros((32, LW), F32)
        for b in range(SB + 1):
            v = fl[b, rows, :] * bcast(e[:, b : b + 1], 32)
            fl[b, rows, :] = v
            al = jnp.where(lane[:32] == b, bcast(v[:, 0:1], 32), al)
            am = jnp.where(lane[:32] == b, bcast(fm[b, rows, 0:1], 32), am)
        cform[1, rows, :] = am
        cform[2, rows, :] = al
        return 0

    def ccopy():
        return remote(colsend, colrecv, cs, cr, (lax.rem(li + 7, 8), sj))

    def columns():
        for f in range(2):
            for t in range(4):
                cols = pl.ds(t * 128, 128)
                colsend[f, :, cols] = cform[f + 1, cols, :].T[:24, :]

        @pl.when(li > 0)
        def _():
            ccopy().start()

        @pl.when(li == 7)
        def _():
            colrecv[...] = jnp.zeros_like(colrecv)

    def column_wait():
        @pl.when(li < 7)
        def _():
            remote(colrecv, colrecv, cs, cr, (lax.rem(li + 1, 8), sj)).wait_recv()
        for f in range(2):
            cbuf[0:24, :] = colrecv[f]
            for t in range(4):
                cols = pl.ds(t * 128, 128)
                cform[f + 1, cols, :] = cbuf[:, cols].T

    def shifted(t, _):
        rows = pl.ds(pl.multiple_of(t * 32, 32), 32)
        for f, (src, dst) in enumerate(((fm, gm), (fl, gl))):
            edge = cform[f + 1, rows, :]
            for b in range(SB + 1):
                rolled = pltpu.roll(src[b, rows, :], LW - 1, 1)
                dst[b, rows, :] = jnp.where(lane[:32] == LW - 1, bcast(edge[:, b : b + 1], 32), rolled)
        return 0

    def march(t, _):
        a0 = pl.multiple_of(t * 32, 32)
        rows = pl.ds(a0, 32)
        after = pl.ds(a0 + 1, 32)
        wb, wa, wl = w[0, rows, :], w[1, rows, :], w[2, rows, :]

        def mixed(f, g, b):
            f0 = f[b, rows, :]
            g0 = g[b, rows, :]
            near_ = f0 + wa * (f[b, after, :] - f0)
            further = g0 + wa * (g[b, after, :] - g0)
            return near_ + wl * (further - near_)

        m0, s0 = mixed(fm, gm, 0), mixed(fl, gl, 0)
        passing = jnp.ones((32, LW), F32)
        part = jnp.zeros((32, LW), F32)
        for b in range(1, SB + 1):
            m1, s1 = mixed(fm, gm, b), mixed(fl, gl, b)
            extinct = m0 + wb * (m1 - m0)
            shaded = s0 + wb * (s1 - s0)
            left = passing * jnp.exp(-extinct)
            part = part + (passing - left) * shaded
            passing = left
            m0, s0 = m1, s1
        place = pl.ds(pl.multiple_of((t // 2) * 32, 32), 32)
        img[t % 2, 0, place, :] = part
        img[t % 2, 1, place, :] = passing
        return 0

    def joined(front, own, other):
        p0 = jnp.where(front, own[0], other[0])
        p1 = jnp.where(front, other[0], own[0])
        t0 = jnp.where(front, own[1], other[1])
        return p0 + t0 * p1, own[1] * other[1]

    def i1copy():
        return remote(img.at[1 - c], imgr, i1s, i1r, device(x, y, z, 1 - c))

    def i2copy():
        return remote(img2.at[1 - zl], img2r, i2s, i2r, device(x, y, zh * 2 + 1 - zl, c))

    def i3copy(d):
        yy = lax.rem(y + d, 4)
        return remote(img3.at[yy], img3r.at[y], i3s.at[d], i3r.at[y], device(x, yy, z, c))

    def image1():
        i1copy().wait_recv()
        for yy in range(4):
            for zz in range(2):
                rows = slice((yy * 2 + zz) * 32, (yy * 2 + zz) * 32 + 32)
                own = (img[c, 0, rows, :], img[c, 1, rows, :])
                a, t = joined(c == 0, own, (imgr[0, rows, :], imgr[1, rows, :]))
                img2[zz, 0, yy * 32 : yy * 32 + 32, :] = a
                img2[zz, 1, yy * 32 : yy * 32 + 32, :] = t
        i2copy().start()

    def image2():
        i2copy().wait_recv()
        for yy in range(4):
            rows = slice(yy * 32, yy * 32 + 32)
            own = (img2[zl, 0, rows, :], img2[zl, 1, rows, :])
            a, t = joined(zl == 0, own, (img2r[0, rows, :], img2r[1, rows, :]))
            img3[yy, 0, :, :] = a
            img3[yy, 1, :, :] = t
        for d in DS:
            i3copy(d).start()
        img3r[y] = img3[y]

    def image3():
        for d in DS:
            src = lax.rem(y + d, 4)
            remote(img3r.at[src], img3r.at[src], i3s.at[d], i3r.at[src], device(x, src, z, c)).wait_recv()
        a, t = img3r[0, 0], img3r[0, 1]
        for yy in range(1, 4):
            a = a + t * img3r[yy, 0]
            t = t * img3r[yy, 1]
        image_out[...] = a
        passing_out[...] = t

    def run(body, lo, hi):
        return lambda: lax.fori_loop(lo, hi, body, 0)

    work = {
        (2, 1): [reach],
        (3, 0): [totals_z],
        (3, 3): [halo_wait],
        (4, 0): [run(scale, 0, 4)],
        (4, 1): [run(scale, 4, 8)],
        (4, 2): [run(scale, 8, 12)],
        (4, 3): [run(scale, 12, 16), columns],
        (5, 0): [totals_x],
        (5, 2): [column_wait],
        (5, 3): [run(shifted, 0, 4)],
        (6, 0): [run(shifted, 4, 8)],
        (6, 1): [run(shifted, 8, 12)],
        (6, 2): [run(shifted, 12, 16)],
        (6, 3): [run(march, 0, 4)],
        (7, 0): [run(march, 4, 8)],
        (7, 1): [run(march, 8, 12)],
        (7, 2): [run(march, 12, 16), lambda: i1copy().start()],
    }
    late = []
    for qq in range(Q):
        for i, d in enumerate((0,) + DS):
            ystep(d, qq)
            late.append((d, qq))
            if len(late) > LAG:
                xsend(*late.pop(0))
            if i == 3 and qq + 2 < Q:
                ysend(qq + 2)
            for task in work.get((qq, i), ()):
                task()
    for item in late:
        xsend(*item)
    image1()
    factors()
    image2()
    image3()

    for i in range(1, 8):
        tcopy(i).wait_send()

    @pl.when(sj > 0)
    def _():
        ecopy().wait_send()

    @pl.when(li > 0)
    def _():
        ccopy().wait_send()

    i1copy().wait_send()
    i2copy().wait_send()
    for d in DS:
        i3copy(d).wait_send()
        tycopy(d).wait_send()
    for d in range(4):
        for kz in range(2):
            zz, cp = tzcopy(d, kz)

            @pl.when(zz != z)
            def _():
                cp.wait_send()

        for j in range(2):
            for kc in range(2):
                at, slot, here, far = txcopy(j, d, kc)

                @pl.when(jnp.logical_not(here))
                def _():
                    far.wait_send()

    def ended(qq, _):
        for d in DS:
            ycopy(d, qq).wait_send()
        for d in range(4):
            for kz in range(2):
                zz, cp = zcopy(d, qq, kz)

                @pl.when(zz != z)
                def _():
                    cp.wait_send()

            for j in range(2):
                for kc in range(2):
                    here, near_, far = xcopies(j, d, qq, kc)

                    @pl.when(here)
                    def _():
                        near_.wait()

                    @pl.when(jnp.logical_not(here))
                    def _():
                        far.wait_send()

        def wait(slot):
            place = bricks_out.at[slot, qq]
            remote(place, place, xs.at[0, 0, 0, 0], xr.at[slot, qq], device(x, y, z, 1 - c)).wait_recv()

        arrivals(wait)
        return 0

    lax.fori_loop(0, Q, ended, 0)


def placed(src, factor, image, passing, out, image_out, passing_out, came, goes, rs, ws):
    def read(i):
        return pltpu.make_async_copy(src.at[:, i // 4, pl.ds((i % 4) * 4, 4)], came.at[i], rs.at[i])

    def write(i):
        return pltpu.make_async_copy(goes.at[i], out.at[pl.ds(i * 4, 4)], ws.at[i])

    for i in range(8):
        read(i).start()
    image_out[...] = image[...]
    passing_out[...] = passing[...]

    def step(i, _):
        read(i).wait()
        f = pltpu.roll(factor[i // 4], lax.rem(LW - (i % 4) * 4, LW), 1)
        for b in range(4):
            for s in range(8):
                at = s * SB + b
                goes[i, b, :, s * LW : (s + 1) * LW] = came[i, s, b] * bcast(f[:, at : at + 1], 32)
        write(i).start()
        return 0

    lax.fori_loop(0, 8, step, 0)
    for i in range(8):
        write(i).wait()


def local(density, albedo, light_in, occupancy, phase, fractions):
    anywhere = pl.BlockSpec(memory_space=pl.ANY)
    vmem = pl.BlockSpec(memory_space=pltpu.VMEM)
    dma = pltpu.SemaphoreType.DMA
    tile = jax.ShapeDtypeStruct((32, LW), F32)
    image, passing, factor, bricks = pl.pallas_call(
        kernel,
        out_shape=(
            tile,
            tile,
            jax.ShapeDtypeStruct((2, 32, LW), F32),
            jax.ShapeDtypeStruct((16, Q, 64, LW), F32),
        ),
        in_specs=[anywhere, anywhere, anywhere, vmem, anywhere, pl.BlockSpec(memory_space=pltpu.SMEM)],
        out_specs=(vmem, vmem, vmem, anywhere),
        scratch_shapes=[
            pltpu.VMEM((SB + 1, PAD, LW), F32),
            pltpu.VMEM((SB + 1, PAD, LW), F32),
            pltpu.VMEM((SB + 1, PAD, LW), F32),
            pltpu.VMEM((SB + 1, PAD, LW), F32),
            pltpu.VMEM((22 * Q, 128, LW), F32),
            pltpu.VMEM((3, NA, LW), F32),
            pltpu.VMEM((NA, LW), F32),
            pltpu.VMEM((3, NA, LW), F32),
            pltpu.VMEM((128, NA), F32),
            pltpu.VMEM((128, NA), F32),
            pltpu.VMEM((8, SB, NA), F32),
            pltpu.VMEM((SB, NA), F32),
            pltpu.VMEM((32, LW), F32),
            pltpu.VMEM((NA, LW), jnp.int32),
            pltpu.VMEM((2, 24, NA), F32),
            pltpu.VMEM((2, 24, NA), F32),
            pltpu.VMEM((15, SB, LW), F32),
            pltpu.VMEM((16, SB, LW), F32),
            pltpu.VMEM((128, LW), F32),
            pltpu.VMEM((2, 2, 256, LW), F32),
            pltpu.VMEM((2, 256, LW), F32),
            pltpu.VMEM((2, 2, 128, LW), F32),
            pltpu.VMEM((2, 128, LW), F32),
            pltpu.VMEM((4, 2, 32, LW), F32),
            pltpu.VMEM((4, 2, 32, LW), F32),
            dma((SB,)), dma((SB,)), dma((3,)),
            dma((2,)), dma((2,)), dma((8,)), dma((8,)), dma(()), dma(()), dma(()), dma(()),
            dma((4, Q)), dma((4, Q)), dma((4, Q, 2)), dma((2, 4, Q)),
            dma((2, 4, Q, 2)), dma((16, Q)), dma((2, Q)),
            dma((4,)), dma((4,)), dma((4, 2)), dma((2, 4)), dma((2, 4, 2)), dma((16,)),
            dma(()), dma(()), dma(()), dma(()), dma((4,)), dma((4,)),
        ],
        compiler_params=pltpu.CompilerParams(
            collective_id=0, has_side_effects=True, vmem_limit_bytes=60 << 20
        ),
    )(density, albedo, light_in, jnp.swapaxes(occupancy, 1, 2), phase, fractions)
    bricks = bricks.reshape(8, 2, 16, 32, LW)
    lit, image, passing = pl.pallas_call(
        placed,
        out_shape=(jax.ShapeDtypeStruct((32, 32, 1024), F32), tile, tile),
        in_specs=[anywhere, vmem, vmem, vmem],
        out_specs=(anywhere, vmem, vmem),
        scratch_shapes=[
            pltpu.VMEM((8, 8, 4, 32, LW), F32),
            pltpu.VMEM((8, 4, 32, 1024), F32),
            dma((8,)),
            dma((8,)),
        ],
    )(bricks, factor, image, passing)
    return image, passing, lit


def solution(mesh):
    return jax.shard_map(
        local,
        mesh=mesh,
        in_specs=(
            P("screen", None, "light"),
            P("screen", None, "light"),
            P(),
            P("screen", None, "light"),
            P(),
            P(),
        ),
        out_specs=(P("screen", "light"), P("screen", "light"), P("light", "screen", None)),
        check_vma=False,
    )
```

```python
import jax
import jax.numpy as jnp
from jax import lax
from jax.experimental import pallas as pl
from jax.experimental.pallas import tpu as pltpu
from jax.sharding import PartitionSpec as P

MESH = pl.DeviceIdType.MESH
F32 = jnp.float32
BRICK = 16
SB = 16
NA = 512
LW = 128
PAD = 520
DS = (1, 3, 2)
Q = 8
LAG = 5


def device(x, y, z, c):
    return (x * 2 + z // 2, y * 4 + (z % 2) * 2 + c)


def bcast(column, rows):
    return jnp.broadcast_to(column, (rows, LW))


def kernel(
    density, albedo, light_in, occ, phase, fractions,
    image_out, passing_out, factor_out, bricks_out,
    fm, fl, gm, gl, big, w, mask, cform, xbuf, cbuf, tg, lin, lin2, ph, colsend, colrecv,
    tb, tin, ftmp, img, imgr, img2, img2r, img3, img3r,
    din, ain, small, hs, hr, ts, tr, es, er, cs, cr, ys, yr, zs, zr, xs, xr, loc,
    tys, tyr, tzs, tzr, txs, txr, i1s, i1r, i2s, i2r, i3s, i3r,
):
    li = lax.axis_index("light")
    sj = lax.axis_index("screen")
    x = li // 2
    zh = li % 2
    y = sj // 4
    zl = (sj // 2) % 2
    c = sj % 2
    z = zh * 2 + zl

    def remote(src, dst, ssem, rsem, dev):
        return pltpu.make_async_remote_copy(
            src_ref=src, dst_ref=dst, send_sem=ssem, recv_sem=rsem,
            device_id=dev, device_id_type=MESH,
        )

    def dload(b):
        return pltpu.make_async_copy(density.at[b], fm.at[b, pl.ds(0, NA)], din.at[b])

    def aload(b):
        return pltpu.make_async_copy(albedo.at[b], fl.at[b, pl.ds(0, NA)], ain.at[b])

    lcopy = pltpu.make_async_copy(light_in.at[pl.ds(sj * SB, SB)], lin, small.at[0])
    pcopy = pltpu.make_async_copy(phase.at[:, pl.ds(li * LW, LW)], ph, small.at[1])
    l2copy = pltpu.make_async_copy(
        light_in.at[pl.ds(li * 32, 32), pl.ds(y * LW, LW)], lin2, small.at[2]
    )
    for b in range(SB):
        dload(b).start()
        aload(b).start()
    lcopy.start()
    l2copy.start()
    pcopy.start()

    barrier = pltpu.get_barrier_semaphore()
    near = [(lax.rem(li + i, 8), sj) for i in range(1, 8)]
    near += [device(x, lax.rem(y + d, 4), z, c) for d in (1, 2, 3)]
    near += [device(lax.rem(x + d, 4), y, z, 1 - c) for d in range(4)]
    near += [device(x, y, lax.rem(z + d, 4), c) for d in (1, 2, 3)]
    near += [(li, lax.rem(sj + 1, 16)), (li, lax.rem(sj + 15, 16))]
    for dev in near:
        pl.semaphore_signal(barrier, inc=1, device_id=dev, device_id_type=MESH)

    lane = lax.broadcasted_iota(jnp.int32, (128, LW), 1)
    o = occ[0].astype(F32)
    tall = (
        lax.broadcasted_iota(jnp.int32, (NA, 32), 0) // BRICK
        == lax.broadcasted_iota(jnp.int32, (NA, 32), 1)
    ).astype(F32)
    tall = lax.dot_general(tall, o, (((1,), (1,)), ((), ())), preferred_element_type=F32)
    spread = (
        lax.broadcasted_iota(jnp.int32, (8, LW), 1) // BRICK
        == lax.broadcasted_iota(jnp.int32, (8, LW), 0)
    ).astype(F32)
    mask[...] = jnp.dot(tall, spread, preferred_element_type=F32)
    r = lax.broadcasted_iota(jnp.int32, (256, 256), 0) % LW
    q = lax.broadcasted_iota(jnp.int32, (256, 256), 1)
    upper = jnp.logical_or(r < q, q >= LW).astype(jnp.bfloat16)

    def unit(d, qq, kz):
        return (d * Q + qq) * 2 + kz

    def held(d):
        return d if d == 0 else d + 3

    def middle(j, d, qq):
        return 14 * Q + (j * 4 + d) * Q + qq

    def ydev(d):
        return device(x, lax.rem(y + d, 4), z, c)

    def ycopy(d, qq):
        return remote(
            big.at[pl.ds(unit(d, qq, 0), 2)], big.at[pl.ds(unit(d + 3, qq, 0), 2)],
            ys.at[d, qq], yr.at[d, qq], ydev(d),
        )

    def ysend(qq):
        for d in DS:
            ycopy(d, qq).start()

    def halo(f, slot):
        return remote(
            f.at[0, pl.ds(0, NA)], f.at[SB, pl.ds(0, NA)], hs.at[slot], hr.at[slot],
            (li, lax.rem(sj + 15, 16)),
        )

    def first(qq):
        for bb in range(2):
            b = qq * 2 + bb
            dload(b).wait()
            aload(b).wait()
            for d in range(4):
                yy = lax.rem(y + d, 4)
                rows = pl.ds(pl.multiple_of(yy * 128, 128), 128)
                m = fm[b, rows, :] * mask[rows, :]
                fm[b, rows, :] = m
                hi = m.astype(jnp.bfloat16)
                lo = (m - hi.astype(F32)).astype(jnp.bfloat16)
                both = jnp.dot(
                    jnp.concatenate([hi, lo], axis=1), upper, preferred_element_type=F32
                )
                v = fl[b, rows, :] * jnp.exp(-both[:, :LW])
                fl[b, rows, :] = v
                for k in range(4):
                    to = (k % 2) * 64 + bb * 32
                    big[unit(d, qq, k // 2), to : to + 32, :] = v[k * 32 : k * 32 + 32, :]
                cform[0, rows, :] = jnp.where(lane == b, both[:, LW:], cform[0, rows, :])

    def weigh(t, _):
        rows = pl.ds(pl.multiple_of(t * 32, 32), 32)
        p = ph[rows, :]
        for k in range(3):
            v = jnp.full((32, LW), fractions[k, 0], F32)
            for level in range(1, 16):
                v = jnp.where(p == level, fractions[k, level], v)
            w[k, rows, :] = v
        return 0

    first(0)
    pcopy.wait()
    lax.fori_loop(0, 16, weigh, 0)
    pl.semaphore_wait(barrier, len(near))
    @pl.when(sj > 0)
    def _():
        halo(fm, 0).start()
        halo(fl, 1).start()

    ysend(0)
    first(1)
    ysend(1)

    @pl.when(sj == 15)
    def _():
        for t in range(4):
            fm[SB, t * 128 : (t + 1) * 128, :] = jnp.zeros((128, LW), F32)
            fl[SB, t * 128 : (t + 1) * 128, :] = jnp.zeros((128, LW), F32)
        xbuf[SB:24, :] = jnp.zeros((8, NA), F32)

    first(2)

    def rest(qq, _):
        first(qq)
        return 0

    lax.fori_loop(3, Q, rest, 0)
    for t in range(4):
        cols = pl.ds(t * 128, 128)
        totals = cform[0, cols, :].T[:SB, :]
        tg[li, :, cols] = totals
        tb[lax.rem(t + 4 - y, 4)] = totals

    def tcopy(i):
        dev = (lax.rem(li + i, 8), sj)
        return remote(tg.at[li], tg.at[li], ts.at[i], tr.at[li], dev)

    def tycopy(d):
        return remote(tb.at[d], tb.at[d + 3], tys.at[d], tyr.at[d], ydev(d))

    for i in (4, 3, 5, 2, 6, 1, 7):
        tcopy(i).start()
    for d in DS:
        tycopy(d).start()

    zero8 = jnp.zeros((8, LW), F32)
    for b in range(SB + 1):
        for ref in (fm, fl, gm, gl):
            ref[b, NA:PAD, :] = zero8

    def zcopy(d, qq, kz):
        zz = 2 * zl + kz
        return zz, remote(
            big.at[unit(held(d), qq, kz)], big.at[middle(zh, d, qq)],
            zs.at[d, qq, kz], zr.at[zh, d, qq], device(x, y, zz, c),
        )

    def tzcopy(d, kz):
        zz = 2 * zl + kz
        return zz, remote(
            tb.at[held(d)], tb.at[7 + zh * 4 + d], tzs.at[d, kz], tzr.at[zh, d],
            device(x, y, zz, c),
        )

    def zsend(d, qq):
        for kz in range(2):
            zz, cp = zcopy(d, qq, kz)

            @pl.when(zz != z)
            def _():
                cp.start()

    def mine(j):
        return (1 - (zl + zh) % 2) * (1 - (j + zh) % 2)

    def zwait(j, d, qq):
        @pl.when(mine(j) == 0)
        def _():
            place = big.at[middle(j, d, qq)]
            remote(place, place, zs.at[d, qq, 0], zr.at[j, d, qq], device(x, y, z, 1 - c)).wait_recv()

    def xto(j, d, kc):
        xx = lax.rem(y + 4 - d, 4)
        here = jnp.logical_and(xx == x, c == kc)
        return (x * 2 + j) * 2 + c, here, device(xx, y, z, kc)

    def xcopies(j, d, qq, kc):
        own = mine(j)
        at = own * unit(held(d), qq, zl) + (1 - own) * middle(j, d, qq)
        src = big.at[at, pl.ds(kc * 64, 64)]
        slot, here, dev = xto(j, d, kc)
        dst = bricks_out.at[slot, qq]
        far = remote(src, dst, xs.at[j, d, qq, kc], xr.at[slot, qq], dev)
        near_ = pltpu.make_async_copy(src, dst, loc.at[j, qq])
        return here, near_, far

    def xsend(d, qq):
        for j in range(2):
            zwait(j, d, qq)
            for kc in range(2):
                here, near_, far = xcopies(j, d, qq, kc)

                @pl.when(here)
                def _():
                    near_.start()

                @pl.when(jnp.logical_not(here))
                def _():
                    far.start()

    def ystep(d, qq):
        if d:
            place = big.at[pl.ds(unit(d + 3, qq, 0), 2)]
            remote(place, place, ys.at[d, qq], yr.at[d, qq], ydev(d)).wait_recv()
        zsend(d, qq)

    def totals_z():
        for d in DS:
            remote(tb.at[d + 3], tb.at[d + 3], tys.at[d], tyr.at[d], ydev(d)).wait_recv()
        for d in range(4):
            for kz in range(2):
                zz, cp = tzcopy(d, kz)

                @pl.when(zz != z)
                def _():
                    cp.start()

    def txcopy(j, d, kc):
        own = mine(j)
        at = own * held(d) + (1 - own) * (7 + j * 4 + d)
        slot, here, dev = xto(j, d, kc)
        return at, slot, here, remote(tb.at[at], tin.at[slot], txs.at[j, d, kc], txr.at[slot], dev)

    def totals_x():
        for j in range(2):
            for d in range(4):
                @pl.when(mine(j) == 0)
                def _():
                    place = tb.at[7 + j * 4 + d]
                    remote(place, place, tzs.at[d, 0], tzr.at[j, d], device(x, y, z, 1 - c)).wait_recv()

                for kc in range(2):
                    at, slot, here, far = txcopy(j, d, kc)

                    @pl.when(here)
                    def _():
                        tin[slot] = tb[at]

                    @pl.when(jnp.logical_not(here))
                    def _():
                        far.start()

    def arrivals(wait):
        for sx in range(4):
            for j in range(2):
                for sc in range(2):
                    slot = (sx * 2 + j) * 2 + sc
                    here = jnp.logical_and(sx == x, sc == c)

                    @pl.when(jnp.logical_not(here))
                    def _():
                        wait(slot)

    def factors():
        def wait(slot):
            remote(tin.at[slot], tin.at[slot], txs.at[0, 0, 0], txr.at[slot], device(x, y, z, 1 - c)).wait_recv()

        arrivals(wait)
        l2copy.wait()
        for cc in range(2):
            above = jnp.zeros((SB, LW), F32)
            for i in range(8):
                ftmp[i * SB : i * SB + SB, :] = lin2[cc * SB : cc * SB + SB, :] * jnp.exp(-above)
                above = above + tin[i * 2 + cc]
            cform[0, 0:128, :] = ftmp[...].T
            factor_out[cc] = cform[0, pl.ds(pl.multiple_of((zl * 2 + c) * 32, 32), 32), :]

    def ecopy():
        return remote(
            xbuf.at[pl.ds(0, 8)], xbuf.at[pl.ds(SB, 8)], es, er, (li, lax.rem(sj + 15, 16))
        )

    def reach():
        lcopy.wait()
        for i in range(1, 8):
            src = lax.rem(li + i, 8)
            remote(tg.at[src], tg.at[src], ts.at[i], tr.at[src], (src, sj)).wait_recv()
        before = jnp.zeros((SB, NA), F32)
        for i in range(8):
            before = before + jnp.where(i < li, tg[i], 0.0)
        xbuf[0:SB, :] = lin[...] * jnp.exp(-before)

        @pl.when(sj > 0)
        def _():
            ecopy().start()

    def halo_wait():
        @pl.when(sj > 0)
        def _():
            halo(fm, 0).wait_send()
            halo(fl, 1).wait_send()

        @pl.when(sj < 15)
        def _():
            for slot, f in enumerate((fm, fl)):
                place = f.at[SB, pl.ds(0, NA)]
                remote(place, place, hs.at[slot], hr.at[slot], (li, lax.rem(sj + 1, 16))).wait_recv()
            place = xbuf.at[pl.ds(SB, 8)]
            remote(place, place, es, er, (li, lax.rem(sj + 1, 16))).wait_recv()

        for t in range(4):
            cols = pl.ds(t * 128, 128)
            cform[0, cols, :] = xbuf[:, cols].T

    def scale(t, _):
        rows = pl.ds(pl.multiple_of(t * 32, 32), 32)
        e = cform[0, rows, :]
        am = jnp.zeros((32, LW), F32)
        al = jnp.zeros((32, LW), F32)
        for b in range(SB + 1):
            v = fl[b, rows, :] * bcast(e[:, b : b + 1], 32)
            fl[b, rows, :] = v
            al = jnp.where(lane[:32] == b, bcast(v[:, 0:1], 32), al)
            am = jnp.where(lane[:32] == b, bcast(fm[b, rows, 0:1], 32), am)
        cform[1, rows, :] = am
        cform[2, rows, :] = al
        return 0

    def ccopy():
        return remote(colsend, colrecv, cs, cr, (lax.rem(li + 7, 8), sj))

    def columns():
        for f in range(2):
            for t in range(4):
                cols = pl.ds(t * 128, 128)
                colsend[f, :, cols] = cform[f + 1, cols, :].T[:24, :]

        @pl.when(li > 0)
        def _():
            ccopy().start()

        @pl.when(li == 7)
        def _():
            colrecv[...] = jnp.zeros_like(colrecv)

    def column_wait():
        @pl.when(li < 7)
        def _():
            remote(colrecv, colrecv, cs, cr, (lax.rem(li + 1, 8), sj)).wait_recv()
        for f in range(2):
            cbuf[0:24, :] = colrecv[f]
            for t in range(4):
                cols = pl.ds(t * 128, 128)
                cform[f + 1, cols, :] = cbuf[:, cols].T

    def shifted(t, _):
        rows = pl.ds(pl.multiple_of(t * 32, 32), 32)
        for f, (src, dst) in enumerate(((fm, gm), (fl, gl))):
            edge = cform[f + 1, rows, :]
            for b in range(SB + 1):
                rolled = pltpu.roll(src[b, rows, :], LW - 1, 1)
                dst[b, rows, :] = jnp.where(lane[:32] == LW - 1, bcast(edge[:, b : b + 1], 32), rolled)
        return 0

    def march(t, _):
        a0 = pl.multiple_of(t * 32, 32)
        rows = pl.ds(a0, 32)
        after = pl.ds(a0 + 1, 32)
        wb, wa, wl = w[0, rows, :], w[1, rows, :], w[2, rows, :]

        def mixed(f, g, b):
            f0 = f[b, rows, :]
            g0 = g[b, rows, :]
            near_ = f0 + wa * (f[b, after, :] - f0)
            further = g0 + wa * (g[b, after, :] - g0)
            return near_ + wl * (further - near_)

        m0, s0 = mixed(fm, gm, 0), mixed(fl, gl, 0)
        passing = jnp.ones((32, LW), F32)
        part = jnp.zeros((32, LW), F32)
        for b in range(1, SB + 1):
            m1, s1 = mixed(fm, gm, b), mixed(fl, gl, b)
            extinct = m0 + wb * (m1 - m0)
            shaded = s0 + wb * (s1 - s0)
            left = passing * jnp.exp(-extinct)
            part = part + (passing - left) * shaded
            passing = left
            m0, s0 = m1, s1
        place = pl.ds(pl.multiple_of((t // 2) * 32, 32), 32)
        img[t % 2, 0, place, :] = part
        img[t % 2, 1, place, :] = passing
        return 0

    def joined(front, own, other):
        p0 = jnp.where(front, own[0], other[0])
        p1 = jnp.where(front, other[0], own[0])
        t0 = jnp.where(front, own[1], other[1])
        return p0 + t0 * p1, own[1] * other[1]

    def i1copy():
        return remote(img.at[1 - c], imgr, i1s, i1r, device(x, y, z, 1 - c))

    def i2copy():
        return remote(img2.at[1 - zl], img2r, i2s, i2r, device(x, y, zh * 2 + 1 - zl, c))

    def i3copy(d):
        yy = lax.rem(y + d, 4)
        return remote(img3.at[yy], img3r.at[y], i3s.at[d], i3r.at[y], device(x, yy, z, c))

    def image1():
        i1copy().wait_recv()
        for yy in range(4):
            for zz in range(2):
                rows = slice((yy * 2 + zz) * 32, (yy * 2 + zz) * 32 + 32)
                own = (img[c, 0, rows, :], img[c, 1, rows, :])
                a, t = joined(c == 0, own, (imgr[0, rows, :], imgr[1, rows, :]))
                img2[zz, 0, yy * 32 : yy * 32 + 32, :] = a
                img2[zz, 1, yy * 32 : yy * 32 + 32, :] = t
        i2copy().start()

    def image2():
        i2copy().wait_recv()
        for yy in range(4):
            rows = slice(yy * 32, yy * 32 + 32)
            own = (img2[zl, 0, rows, :], img2[zl, 1, rows, :])
            a, t = joined(zl == 0, own, (img2r[0, rows, :], img2r[1, rows, :]))
            img3[yy, 0, :, :] = a
            img3[yy, 1, :, :] = t
        for d in DS:
            i3copy(d).start()
        img3r[y] = img3[y]

    def image3():
        for d in DS:
            src = lax.rem(y + d, 4)
            remote(img3r.at[src], img3r.at[src], i3s.at[d], i3r.at[src], device(x, src, z, c)).wait_recv()
        a, t = img3r[0, 0], img3r[0, 1]
        for yy in range(1, 4):
            a = a + t * img3r[yy, 0]
            t = t * img3r[yy, 1]
        image_out[...] = a
        passing_out[...] = t

    def run(body, lo, hi):
        return lambda: lax.fori_loop(lo, hi, body, 0)

    work = {
        (2, 1): [reach],
        (3, 0): [totals_z],
        (3, 3): [halo_wait],
        (4, 0): [run(scale, 0, 4)],
        (4, 1): [run(scale, 4, 8)],
        (4, 2): [run(scale, 8, 12)],
        (4, 3): [run(scale, 12, 16), columns],
        (5, 0): [totals_x, column_wait],
        (5, 1): [run(shifted, 0, 4)],
        (5, 2): [run(shifted, 4, 8)],
        (5, 3): [run(shifted, 8, 12)],
        (6, 0): [run(shifted, 12, 16)],
        (6, 1): [run(march, 0, 4)],
        (6, 2): [run(march, 4, 8)],
        (6, 3): [run(march, 8, 12)],
        (7, 0): [run(march, 12, 16), lambda: i1copy().start()],
        (7, 2): [image1],
    }
    late = []
    for qq in range(Q):
        for i, d in enumerate((0,) + DS):
            ystep(d, qq)
            late.append((d, qq))
            if len(late) > LAG:
                xsend(*late.pop(0))
            if i == 3 and qq + 2 < Q:
                ysend(qq + 2)
            for task in work.get((qq, i), ()):
                task()
    for item in late:
        xsend(*item)
    image2()
    factors()
    image3()

    for i in range(1, 8):
        tcopy(i).wait_send()

    @pl.when(sj > 0)
    def _():
        ecopy().wait_send()

    @pl.when(li > 0)
    def _():
        ccopy().wait_send()

    i1copy().wait_send()
    i2copy().wait_send()
    for d in DS:
        i3copy(d).wait_send()
        tycopy(d).wait_send()
    for d in range(4):
        for kz in range(2):
            zz, cp = tzcopy(d, kz)

            @pl.when(zz != z)
            def _():
                cp.wait_send()

        for j in range(2):
            for kc in range(2):
                at, slot, here, far = txcopy(j, d, kc)

                @pl.when(jnp.logical_not(here))
                def _():
                    far.wait_send()

    def ended(qq, _):
        for d in DS:
            ycopy(d, qq).wait_send()
        for d in range(4):
            for kz in range(2):
                zz, cp = zcopy(d, qq, kz)

                @pl.when(zz != z)
                def _():
                    cp.wait_send()

            for j in range(2):
                for kc in range(2):
                    here, near_, far = xcopies(j, d, qq, kc)

                    @pl.when(here)
                    def _():
                        near_.wait()

                    @pl.when(jnp.logical_not(here))
                    def _():
                        far.wait_send()

        def wait(slot):
            place = bricks_out.at[slot, qq]
            remote(place, place, xs.at[0, 0, 0, 0], xr.at[slot, qq], device(x, y, z, 1 - c)).wait_recv()

        arrivals(wait)
        return 0

    lax.fori_loop(0, Q, ended, 0)


def placed(src, factor, image, passing, out, image_out, passing_out, came, goes, rs, ws):
    def read(i):
        return pltpu.make_async_copy(src.at[:, i // 4, pl.ds((i % 4) * 4, 4)], came.at[i], rs.at[i])

    def write(i):
        return pltpu.make_async_copy(goes.at[i], out.at[pl.ds(i * 4, 4)], ws.at[i])

    for i in range(8):
        read(i).start()
    image_out[...] = image[...]
    passing_out[...] = passing[...]

    def step(i, _):
        read(i).wait()
        f = pltpu.roll(factor[i // 4], lax.rem(LW - (i % 4) * 4, LW), 1)
        for b in range(4):
            for s in range(8):
                at = s * SB + b
                goes[i, b, :, s * LW : (s + 1) * LW] = came[i, s, b] * bcast(f[:, at : at + 1], 32)
        write(i).start()
        return 0

    lax.fori_loop(0, 8, step, 0)
    for i in range(8):
        write(i).wait()


def local(density, albedo, light_in, occupancy, phase, fractions):
    anywhere = pl.BlockSpec(memory_space=pl.ANY)
    vmem = pl.BlockSpec(memory_space=pltpu.VMEM)
    dma = pltpu.SemaphoreType.DMA
    tile = jax.ShapeDtypeStruct((32, LW), F32)
    image, passing, factor, bricks = pl.pallas_call(
        kernel,
        out_shape=(
            tile,
            tile,
            jax.ShapeDtypeStruct((2, 32, LW), F32),
            jax.ShapeDtypeStruct((16, Q, 64, LW), F32),
        ),
        in_specs=[anywhere, anywhere, anywhere, vmem, anywhere, pl.BlockSpec(memory_space=pltpu.SMEM)],
        out_specs=(vmem, vmem, vmem, anywhere),
        scratch_shapes=[
            pltpu.VMEM((SB + 1, PAD, LW), F32),
            pltpu.VMEM((SB + 1, PAD, LW), F32),
            pltpu.VMEM((SB + 1, PAD, LW), F32),
            pltpu.VMEM((SB + 1, PAD, LW), F32),
            pltpu.VMEM((22 * Q, 128, LW), F32),
            pltpu.VMEM((3, NA, LW), F32),
            pltpu.VMEM((NA, LW), F32),
            pltpu.VMEM((3, NA, LW), F32),
            pltpu.VMEM((128, NA), F32),
            pltpu.VMEM((128, NA), F32),
            pltpu.VMEM((8, SB, NA), F32),
            pltpu.VMEM((SB, NA), F32),
            pltpu.VMEM((32, LW), F32),
            pltpu.VMEM((NA, LW), jnp.int32),
            pltpu.VMEM((2, 24, NA), F32),
            pltpu.VMEM((2, 24, NA), F32),
            pltpu.VMEM((15, SB, LW), F32),
            pltpu.VMEM((16, SB, LW), F32),
            pltpu.VMEM((128, LW), F32),
            pltpu.VMEM((2, 2, 256, LW), F32),
            pltpu.VMEM((2, 256, LW), F32),
            pltpu.VMEM((2, 2, 128, LW), F32),
            pltpu.VMEM((2, 128, LW), F32),
            pltpu.VMEM((4, 2, 32, LW), F32),
            pltpu.VMEM((4, 2, 32, LW), F32),
            dma((SB,)), dma((SB,)), dma((3,)),
            dma((2,)), dma((2,)), dma((8,)), dma((8,)), dma(()), dma(()), dma(()), dma(()),
            dma((4, Q)), dma((4, Q)), dma((4, Q, 2)), dma((2, 4, Q)),
            dma((2, 4, Q, 2)), dma((16, Q)), dma((2, Q)),
            dma((4,)), dma((4,)), dma((4, 2)), dma((2, 4)), dma((2, 4, 2)), dma((16,)),
            dma(()), dma(()), dma(()), dma(()), dma((4,)), dma((4,)),
        ],
        compiler_params=pltpu.CompilerParams(
            collective_id=0, has_side_effects=True, vmem_limit_bytes=60 << 20
        ),
    )(density, albedo, light_in, jnp.swapaxes(occupancy, 1, 2), phase, fractions)
    bricks = bricks.reshape(8, 2, 16, 32, LW)
    lit, image, passing = pl.pallas_call(
        placed,
        out_shape=(jax.ShapeDtypeStruct((32, 32, 1024), F32), tile, tile),
        in_specs=[anywhere, vmem, vmem, vmem],
        out_specs=(anywhere, vmem, vmem),
        scratch_shapes=[
            pltpu.VMEM((8, 8, 4, 32, LW), F32),
            pltpu.VMEM((8, 4, 32, 1024), F32),
            dma((8,)),
            dma((8,)),
        ],
    )(bricks, factor, image, passing)
    return image, passing, lit


def solution(mesh):
    return jax.shard_map(
        local,
        mesh=mesh,
        in_specs=(
            P("screen", None, "light"),
            P("screen", None, "light"),
            P(),
            P("screen", None, "light"),
            P(),
            P(),
        ),
        out_specs=(P("screen", "light"), P("screen", "light"), P("light", "screen", None)),
        check_vma=False,
    )
```
